32 devices in a mesh: dp: 8 (over z, x), mp: 4 (over y, core).
Axes of the slice: x: 2, y: 2, z: 4, core: 2. Of those that a mesh axis runs over, the one named last changes fastest.
Arguments:
- activations: bfloat16 [1024, 1024], P('dp'), may hold values from -6 to 6
- cotangents: bfloat16 [1024, 4096], P('dp', 'mp'), may hold values from -1200 to 1200
- owners: int32 [4], replicated, may hold values from 0 to 7, as said below
Outputs:
- update: bfloat16 [1024, 4096], P('dp', 'mp')
- roots: float32 [4096, 2048], P('dp', 'mp')
- graft: float32 [], replicated
The draws below stay inside these ranges and needn't reach their ends.
Inputs may be any that keep to these rules, and one draw needn't show every extreme that they name: The left root of block b is computed at dp index owners[b] and its right root at owners[b] with its lowest bit flipped; every dp index computes exactly one root.
All inputs are finite; a program needn't handle non-finite values.
Results may differ from the reference program's by a relative error of at most 0.00045.
Values may be sent and summed in bfloat16 or wider, within the bound.
A program may use at most 64 MiB of HBM per device.

```python
import math
import jax
import jax.numpy as jnp
from jax import lax

B = 512
CB = 2
ITERS = 3
RB = 2
NB = 4
DIN = 1024
DOUT = 4096
TOKENS = 1024
N_DP = 8
N_MP = 4


def draw_owners(key, part):
    pair_key = jax.random.fold_in(key, 11)
    side_key = jax.random.fold_in(key, 23)
    pairs = jax.random.permutation(pair_key, NB)
    sides = jax.random.randint(side_key, (NB,), 0, 2)
    return (2 * pairs + sides).astype(jnp.int32)


def draw_cotangents(key, part):
    base_key = jax.random.fold_in(key, 31)
    group_key = jax.random.fold_in(key, 37)
    pick_key = jax.random.fold_in(key, 41)
    base = jax.random.truncated_normal(base_key, -6.0, 6.0, (TOKENS, DOUT), jnp.float32)
    group_ids = jnp.arange(N_MP, dtype=jnp.int32)
    chosen = jax.random.randint(pick_key, (), 0, N_MP)
    group_scale = jnp.exp(jax.random.uniform(group_key, (N_MP,), jnp.float32, jnp.log(0.5), jnp.log(2.0)))
    group_scale = jnp.where(group_ids == chosen, 6.0, group_scale)
    column_scale = jnp.repeat(group_scale, CB * B)
    return (base * column_scale[None, :]).astype(jnp.bfloat16)


def block_levels(rng, dims, split, least, high):
    factor_of = 1.0
    for position, blocks in split:
        draws = jax.random.uniform(jax.random.fold_in(jax.random.fold_in(rng, 6), position), (blocks,), jnp.float32, least / len(split), high / len(split))
        factor_of = factor_of * jnp.repeat(jnp.exp(draws), dims[position] // blocks).reshape((-1,) + (1,) * (len(dims) - 1 - position))
    return factor_of


def normal_values(rng, shape, spread, most, pieces=(), kind=jnp.bfloat16):
    array = spread * jax.random.normal(rng, shape, jnp.float32)
    if pieces:
        array = array * block_levels(rng, shape, pieces, -0.22, 0.18)
    return jnp.clip(array, -most, most).astype(kind)


def setup_inputs(seed: int = 0) -> dict:
    splits = jax.random.split(jax.random.key(seed), 4)
    return {
        "activations": normal_values(splits[0], (TOKENS, DIN), 1.0, 6.0, ((0, 8),)),
        "cotangents": draw_cotangents(jax.random.fold_in(splits[3], 71), 0),
        "owners": draw_owners(jax.random.fold_in(splits[3], 71), 0),
    }


def product(left, right):
    return jnp.dot(left, right, precision=lax.Precision.HIGHEST, preferred_element_type=jnp.float32)

def statistic_of(operand):
    gram = product(operand, operand.T)
    ridge = 0.1 * (jnp.sum(operand * operand) / operand.shape[0] + 1.0)
    return gram + ridge * jnp.eye(operand.shape[0], dtype=jnp.float32)

def inverse_root(statistic):
    eye_matrix = jnp.eye(statistic.shape[0], dtype=jnp.float32)
    magnitude = jnp.sqrt(jnp.sum(statistic * statistic))
    current = statistic / magnitude
    result = eye_matrix
    for step in range(ITERS):
        factor = (5.0 * eye_matrix - current) * 0.25
        if step == 0:
            result = factor * magnitude ** (-0.25)
        else:
            result = product(result, factor)
        if step + 1 < ITERS:
            square = product(factor, factor)
            current = product(product(square, square), current)
    return result

def one_block(grad_block):
    left_root = inverse_root(statistic_of(grad_block))
    right_root = inverse_root(statistic_of(grad_block.T))
    precond = product(left_root, product(grad_block, right_root))
    return (left_root, right_root, precond)

def reference(activations, cotangents, owners):
    gradient = jnp.dot(activations.astype(jnp.float32).T, cotangents.astype(jnp.float32), precision=lax.Precision.HIGHEST, preferred_element_type=jnp.float32) / math.sqrt(TOKENS)
    columns_all = N_MP * CB
    blocks = gradient.reshape(RB, B, columns_all, B).transpose(0, 2, 1, 3).reshape(RB * columns_all, B, B)
    left_all, right_all, precond_all = lax.map(one_block, blocks)
    grad_total = jnp.sum(gradient * gradient)
    precond_total = jnp.sum(precond_all * precond_all)
    graft = jnp.sqrt(grad_total / jnp.maximum(precond_total, 1.0))
    whole = precond_all.reshape(RB, columns_all, B, B).transpose(0, 2, 1, 3).reshape(DIN, DOUT)
    update = (graft * whole).astype(jnp.bfloat16)
    index_dp = jnp.arange(N_DP, dtype=jnp.int32)
    partner = owners + 1 - 2 * (owners % 2)
    left_match = owners[None, :] == index_dp[:, None]
    right_match = partner[None, :] == index_dp[:, None]
    block_ids = jnp.arange(NB, dtype=jnp.int32)
    owned = lax.optimization_barrier(jnp.sum(jnp.where(left_match | right_match, block_ids[None, :], 0), axis=1)).astype(jnp.int32)
    is_left = jnp.any(left_match, axis=1)
    row_block = owned // CB
    col_block = owned % CB
    column_ids = jnp.arange(N_MP, dtype=jnp.int32)[None, :] * CB + col_block[:, None]
    flat_ids = (row_block[:, None] * columns_all + column_ids).astype(jnp.int32)
    picked = jnp.where(is_left[:, None, None, None], left_all[flat_ids], right_all[flat_ids])
    roots = picked.transpose(0, 2, 1, 3).reshape(N_DP * B, N_MP * B)
    return (update, roots, graft)
```

```python
import functools
import math

import jax
import jax.numpy as jnp
from jax import lax
from jax.experimental import pallas as pl
from jax.experimental.pallas import tpu as pltpu
from jax.sharding import PartitionSpec as P

B = 512
CB = 2
MESH = pl.DeviceIdType.MESH


def gather_kernel(dp, mp, a_sel, c_sel, a_all, c_all, az_send, ax_send, am_send, cz_send, cx_send, a_recv, c_recv):
    pairs = dp // 2
    me = lax.axis_index("dp")
    col = lax.axis_index("mp")
    pair = me // 2
    side = me % 2
    across = 2 * pair + 1 - side

    def source(k):
        return 2 * lax.rem(pair + k, pairs) + side

    barrier = pltpu.get_barrier_semaphore()
    for k in range(1, pairs):
        pl.semaphore_signal(barrier, inc=1, device_id=(source(k), col), device_id_type=MESH)
    pl.semaphore_signal(barrier, inc=1, device_id=(across, col), device_id_type=MESH)
    for k in range(1, mp):
        pl.semaphore_signal(barrier, inc=1, device_id=(me, lax.rem(col + k, mp)), device_id_type=MESH)
    pl.semaphore_wait(barrier, pairs - 1 + 1 + mp - 1)

    def a_pair(k):
        dest = lax.rem(pair + k, pairs)
        return pltpu.make_async_remote_copy(
            a_sel.at[dest], a_all.at[me, col], az_send.at[k], a_recv.at[me, col], (source(k), col), MESH)

    def c_pair(k):
        dest = lax.rem(pair + k, pairs)
        return pltpu.make_async_remote_copy(
            c_sel.at[dest], c_all.at[me], cz_send.at[k], c_recv.at[me], (source(k), col), MESH)

    def a_across(k):
        src = source(k)
        ref = a_sel.at[pair] if k == 0 else a_all.at[src, col]
        return pltpu.make_async_remote_copy(
            ref, a_all.at[src, col], ax_send.at[k], a_recv.at[src, col], (across, col), MESH)

    def c_across(k):
        src = source(k)
        ref = c_sel.at[pair] if k == 0 else c_all.at[src]
        return pltpu.make_async_remote_copy(
            ref, c_all.at[src], cx_send.at[k], c_recv.at[src], (across, col), MESH)

    def a_mp(src, k, own=False):
        ref = a_sel.at[pair] if own else a_all.at[src, col]
        return pltpu.make_async_remote_copy(
            ref, a_all.at[src, col], am_send.at[src, k], a_recv.at[src, col], (me, lax.rem(col + k, mp)), MESH)

    def start_mp(src):
        @pl.loop(1, mp)
        def _(k):
            a_mp(src, k).start()

    def a_arrived(src, who):
        pltpu.make_async_copy(a_all.at[src, who], a_all.at[src, who], a_recv.at[src, who]).wait()

    def c_arrived(src):
        pltpu.make_async_copy(c_all.at[src], c_all.at[src], c_recv.at[src]).wait()

    order = list(range(1, pairs))
    a_across(0).start()
    for k in order:
        a_pair(k).start()
    c_across(0).start()
    for k in order:
        c_pair(k).start()

    @pl.loop(1, mp)
    def _(k):
        a_mp(me, k, own=True).start()

    a_all[me, col] = a_sel[pair]
    c_all[me] = c_sel[pair]
    for k in order:
        a_arrived(source(k), col)
        a_across(k).start()
        start_mp(source(k))
    for k in range(pairs):
        other = source(k) + 1 - 2 * side
        a_arrived(other, col)
        start_mp(other)
    for k in order:
        c_arrived(source(k))
        c_across(k).start()

    @pl.loop(0, dp)
    def _(src):
        @pl.loop(1, mp)
        def _(k):
            a_arrived(src, lax.rem(col + k, mp))
            a_mp(src, k).wait_send()

    for k in range(pairs):
        c_arrived(source(k) + 1 - 2 * side)
    for k in range(pairs):
        a_across(k).wait_send()
        c_across(k).wait_send()
    for k in order:
        a_pair(k).wait_send()
        c_pair(k).wait_send()


def finish_kernel(dp, mp, owners, stats, pre, update, graft_ref, slots, out, got, m_send, m_recv, d_send, d_recv, u_send, u_recv):
    pairs = dp // 2
    halves = pre.shape[0]
    me = lax.axis_index("dp")
    col = lax.axis_index("mp")
    pair = me // 2
    side = me % 2

    barrier = pltpu.get_barrier_semaphore()
    for k in range(1, dp):
        pl.semaphore_signal(barrier, inc=1, device_id=(lax.rem(me + k, dp), col), device_id_type=MESH)
    for k in range(1, mp):
        pl.semaphore_signal(barrier, inc=1, device_id=(me, lax.rem(col + k, mp)), device_id_type=MESH)
    slots[me, col] = stats[...]
    pl.semaphore_wait(barrier, dp - 1 + mp - 1)

    def over_mp(k):
        return pltpu.make_async_remote_copy(
            stats, slots.at[me, col], m_send.at[k], m_recv.at[col], (me, lax.rem(col + k, mp)), MESH)

    def over_dp(k):
        return pltpu.make_async_remote_copy(
            slots.at[me], slots.at[me], d_send.at[k], d_recv.at[me], (lax.rem(me + k, dp), col), MESH)

    for k in range(1, mp):
        over_mp(k).start()
    for k in range(1, mp):
        who = lax.rem(col + k, mp)
        pltpu.make_async_copy(stats, stats, m_recv.at[who]).wait()
    for k in range(1, dp):
        over_dp(k).start()
    for k in range(1, dp):
        who = lax.rem(me + k, dp)
        pltpu.make_async_copy(slots.at[who], slots.at[who], d_recv.at[who]).wait()
    totals = jnp.sum(slots[...].reshape(dp * mp, *stats.shape), axis=0)
    grad_total = totals[0:1, 0:1]
    pre_total = totals[1:2, 0:1]
    graft = jnp.sqrt(grad_total / jnp.maximum(pre_total, 1.0))
    graft_ref[...] = jnp.broadcast_to(graft, graft_ref.shape)
    out[...] = (pre[...] * graft[None]).astype(jnp.bfloat16)

    def piece(k):
        dest = lax.rem(pair + k, pairs)
        return pltpu.make_async_remote_copy(
            out.at[dest % halves], got.at[pair], u_send.at[k], u_recv.at[pair], (2 * dest + side, col), MESH)

    for k in range(1, pairs):
        piece(k).start()
    got[pair] = out[pair % halves]
    for k in range(1, pairs):
        who = lax.rem(pair + k, pairs)
        pltpu.make_async_copy(got.at[who], got.at[who], u_recv.at[who]).wait()
    for c in range(CB):
        holder = owners[(pair // halves) * CB + c] // 2
        update[:, c * B : (c + 1) * B] = got[holder]
    for k in range(1, mp):
        over_mp(k).wait_send()
    for k in range(1, dp):
        over_dp(k).wait_send()
    for k in range(1, pairs):
        piece(k).wait_send()


def product(left, right):
    return jnp.matmul(left, right, precision=lax.Precision.HIGH, preferred_element_type=jnp.float32)


def inverse_roots(stat):
    eye = jnp.eye(B, dtype=jnp.float32)
    size = jnp.sqrt(jnp.sum(stat * stat))
    m = stat / size
    m2 = product(m, m)
    f = (5.0 * eye - m) * 0.25
    f2 = (25.0 * eye - 10.0 * m + m2) * 0.0625
    mf = (5.0 * m - m2) * 0.25
    y = (5.0 * f - product(product(f2, f2), mf)) * 0.25
    my = product(m, y)
    y2 = product(y, y)
    return (5.0 * y - product(product(y2, y2), my)) * (0.25 * size ** (-0.25))


def on_device(activations, cotangents, owners):
    dp = lax.axis_size("dp")
    mp = lax.axis_size("mp")
    me = lax.axis_index("dp")
    col = lax.axis_index("mp")
    pairs = dp // 2
    tokens, features = activations.shape
    part = tokens // mp
    ids = jnp.arange(owners.shape[0], dtype=jnp.int32)
    pair_ids = jnp.arange(pairs, dtype=jnp.int32)
    block_of = jnp.sum(jnp.where(owners[None, :] // 2 == pair_ids[:, None], ids[None, :], 0), axis=1)
    my_block = block_of[me // 2]
    my_left = owners[my_block] == me

    mine = lax.dynamic_slice_in_dim(activations, col * part, part, 0)
    a_sel = jnp.take(mine.reshape(part, features // B, B).transpose(1, 0, 2), block_of // CB, axis=0)
    c_sel = jnp.take(cotangents.reshape(tokens, CB, B).transpose(1, 0, 2), block_of % CB, axis=0)
    vmem = pl.BlockSpec(memory_space=pltpu.VMEM)
    dma = pltpu.SemaphoreType.DMA
    a_all, c_all = pl.pallas_call(
        functools.partial(gather_kernel, dp, mp),
        out_shape=(
            jax.ShapeDtypeStruct((dp, mp, part, B), jnp.bfloat16),
            jax.ShapeDtypeStruct((dp, tokens, B), jnp.bfloat16),
        ),
        in_specs=[vmem] * 2,
        out_specs=(vmem, vmem),
        scratch_shapes=[
            dma((pairs,)), dma((pairs,)), dma((dp, mp)), dma((pairs,)), dma((pairs,)), dma((dp, mp)), dma((dp,)),
        ],
        compiler_params=pltpu.CompilerParams(collective_id=0, has_side_effects=True),
    )(a_sel, c_sel)

    all_tokens = dp * tokens
    gradient = lax.dot_general(
        a_all.reshape(all_tokens, B), c_all.reshape(all_tokens, B), (((0,), (0,)), ((), ())),
        preferred_element_type=jnp.float32,
    ) / math.sqrt(all_tokens)
    ridge = 0.1 * (jnp.sum(gradient * gradient) / B + 1.0) * jnp.eye(B, dtype=jnp.float32)
    left = inverse_roots(product(gradient, gradient.T) + ridge)
    right = inverse_roots(product(gradient.T, gradient) + ridge)
    root = jnp.where(my_left, left, right)

    rows = features // dp
    halves = B // rows // 2

    def my_rows(matrix):
        return lax.dynamic_index_in_dim(matrix.reshape(halves, 2, rows, B), me % 2, 1, keepdims=False)

    pre = product(product(my_rows(left).reshape(halves * rows, B), gradient), right)
    sums = jnp.stack([jnp.sum(jnp.square(my_rows(gradient))), jnp.sum(pre * pre)])
    stats = jnp.zeros((8, 128), jnp.float32).at[0:2, :].set(sums[:, None])
    update, graft = pl.pallas_call(
        functools.partial(finish_kernel, dp, mp),
        out_shape=(
            jax.ShapeDtypeStruct((rows, CB * B), jnp.bfloat16),
            jax.ShapeDtypeStruct((8, 128), jnp.float32),
        ),
        in_specs=[pl.BlockSpec(memory_space=pltpu.SMEM), vmem, vmem],
        out_specs=(vmem, vmem),
        scratch_shapes=[
            pltpu.VMEM((dp, mp, 8, 128), jnp.float32),
            pltpu.VMEM((halves, rows, B), jnp.bfloat16),
            pltpu.VMEM((pairs, rows, B), jnp.bfloat16),
            dma((mp,)), dma((mp,)), dma((dp,)), dma((dp,)), dma((pairs,)), dma((pairs,)),
        ],
        compiler_params=pltpu.CompilerParams(collective_id=1, has_side_effects=True),
    )(owners, stats, pre.reshape(halves, rows, B))
    return (update, root, graft[0, 0])


def solution(mesh):
    return jax.shard_map(
        on_device,
        mesh=mesh,
        in_specs=(P("dp", None), P("dp", "mp"), P()),
        out_specs=(P("dp", "mp"), P("dp", "mp"), P()),
        check_vma=False,
    )
```

```python
import functools
import math

import jax
import jax.numpy as jnp
from jax import lax
from jax.experimental import pallas as pl
from jax.experimental.pallas import tpu as pltpu
from jax.sharding import PartitionSpec as P

B = 512
CB = 2
MESH = pl.DeviceIdType.MESH


def gather_kernel(dp, mp, owners, acts, cots, grad, oriented, a_sel, c_sel, a_all, c_all, az_send, ax_send, am_send, cz_send, cx_send, a_recv, c_recv):
    pairs = dp // 2
    me = lax.axis_index("dp")
    col = lax.axis_index("mp")
    pair = me // 2
    side = me % 2
    across = 2 * pair + 1 - side

    def source(k):
        return 2 * lax.rem(pair + k, pairs) + side

    barrier = pltpu.get_barrier_semaphore()
    for k in range(1, pairs):
        pl.semaphore_signal(barrier, inc=1, device_id=(source(k), col), device_id_type=MESH)
    pl.semaphore_signal(barrier, inc=1, device_id=(across, col), device_id_type=MESH)
    for k in range(1, mp):
        pl.semaphore_signal(barrier, inc=1, device_id=(me, lax.rem(col + k, mp)), device_id_type=MESH)

    def block_of(which):
        held = [jnp.where(owners[b] // 2 == which, b, 0) for b in range(owners.shape[0])]
        return functools.reduce(jnp.add, held)

    def chosen(wide, which):
        parts = [
            wide[:, n * B : (n + 1) * B] * jnp.where(which == n, 1.0, 0.0).astype(wide.dtype)
            for n in range(wide.shape[1] // B)
        ]
        return functools.reduce(jnp.add, parts)

    part = a_sel.shape[1]
    scale = 1.0 / math.sqrt(dp * cots.shape[0])
    for dest in range(pairs):
        block = block_of(dest)
        row_start = pl.multiple_of(col * part, part)
        mine = acts[pl.ds(row_start, part), :]
        a_sel[dest] = chosen(mine, block // CB)
        c_sel[dest] = chosen(cots[...], block % CB)
    is_left = functools.reduce(
        jnp.add, [jnp.where(owners[b] == me, 1.0, 0.0) for b in range(owners.shape[0])])
    a_all[me, col] = a_sel[pair]
    c_all[me] = c_sel[pair]
    pl.semaphore_wait(barrier, pairs - 1 + 1 + mp - 1)

    def a_pair(k):
        dest = lax.rem(pair + k, pairs)
        return pltpu.make_async_remote_copy(
            a_sel.at[dest], a_all.at[me, col], az_send.at[k], a_recv.at[me, col], (source(k), col), MESH)

    def c_pair(k):
        dest = lax.rem(pair + k, pairs)
        return pltpu.make_async_remote_copy(
            c_sel.at[dest], c_all.at[me], cz_send.at[k], c_recv.at[me], (source(k), col), MESH)

    def a_across(k):
        src = source(k)
        ref = a_sel.at[pair] if k == 0 else a_all.at[src, col]
        return pltpu.make_async_remote_copy(
            ref, a_all.at[src, col], ax_send.at[k], a_recv.at[src, col], (across, col), MESH)

    def c_across(k):
        src = source(k)
        ref = c_sel.at[pair] if k == 0 else c_all.at[src]
        return pltpu.make_async_remote_copy(
            ref, c_all.at[src], cx_send.at[k], c_recv.at[src], (across, col), MESH)

    def a_mp(src, k, own=False):
        ref = a_sel.at[pair] if own else a_all.at[src, col]
        return pltpu.make_async_remote_copy(
            ref, a_all.at[src, col], am_send.at[src, k], a_recv.at[src, col], (me, lax.rem(col + k, mp)), MESH)

    def start_mp(src):
        @pl.loop(1, mp)
        def _(k):
            a_mp(src, k).start()

    def a_arrived(src, who):
        pltpu.make_async_copy(a_all.at[src, who], a_all.at[src, who], a_recv.at[src, who]).wait()

    def c_arrived(src):
        pltpu.make_async_copy(c_all.at[src], c_all.at[src], c_recv.at[src]).wait()

    order = list(range(1, pairs))
    a_across(0).start()
    for k in order:
        a_pair(k).start()
    c_across(0).start()
    for k in order:
        c_pair(k).start()

    @pl.loop(1, mp)
    def _(k):
        a_mp(me, k, own=True).start()

    for k in order:
        a_arrived(source(k), col)
        a_across(k).start()
        start_mp(source(k))
    for k in range(pairs):
        other = source(k) + 1 - 2 * side
        a_arrived(other, col)
        start_mp(other)
    def a_complete(src):
        @pl.loop(1, mp)
        def _(k):
            a_arrived(src, lax.rem(col + k, mp))

    def accumulate(k):
        base = 2 * lax.rem(pair + k, pairs)
        a_complete(base)
        a_complete(base + 1)
        c_arrived(source(k) + 1 - 2 * side)
        tokens = 2 * cots.shape[0]
        a = a_all[pl.ds(base, 2)].reshape(tokens, B)
        c = c_all[pl.ds(base, 2)].reshape(tokens, B)
        keep = is_left.astype(a.dtype)
        swap = (1.0 - is_left).astype(a.dtype)
        first = a * keep + c * swap
        second = c * keep + a * swap
        dims = (((0,), (0,)), ((), ()))
        add = lax.dot_general(a, c, dims, preferred_element_type=jnp.float32) * scale
        add_oriented = lax.dot_general(first, second, dims, preferred_element_type=jnp.float32) * scale
        if k == 0:
            grad[...] = add
            oriented[...] = add_oriented
        else:
            grad[...] += add
            oriented[...] += add_oriented

    for k in order:
        c_arrived(source(k))
        c_across(k).start()
        accumulate(k - 1)
    accumulate(pairs - 1)

    @pl.loop(0, dp)
    def _(src):
        @pl.loop(1, mp)
        def _(k):
            a_mp(src, k).wait_send()

    for k in range(pairs):
        a_across(k).wait_send()
        c_across(k).wait_send()
    for k in order:
        a_pair(k).wait_send()
        c_pair(k).wait_send()


def finish_kernel(dp, mp, owners, stats, pre, update, graft_ref, slots, out, got, m_send, m_recv, d_send, d_recv, u_send, u_recv):
    pairs = dp // 2
    halves = pre.shape[0]
    me = lax.axis_index("dp")
    col = lax.axis_index("mp")
    pair = me // 2
    side = me % 2

    barrier = pltpu.get_barrier_semaphore()
    for k in range(1, dp):
        pl.semaphore_signal(barrier, inc=1, device_id=(lax.rem(me + k, dp), col), device_id_type=MESH)
    for k in range(1, mp):
        pl.semaphore_signal(barrier, inc=1, device_id=(me, lax.rem(col + k, mp)), device_id_type=MESH)
    slots[me, col] = stats[...]
    pl.semaphore_wait(barrier, dp - 1 + mp - 1)

    def over_mp(k):
        return pltpu.make_async_remote_copy(
            stats, slots.at[me, col], m_send.at[k], m_recv.at[col], (me, lax.rem(col + k, mp)), MESH)

    def over_dp(k):
        return pltpu.make_async_remote_copy(
            slots.at[me], slots.at[me], d_send.at[k], d_recv.at[me], (lax.rem(me + k, dp), col), MESH)

    for k in range(1, mp):
        over_mp(k).start()
    for k in range(1, mp):
        who = lax.rem(col + k, mp)
        pltpu.make_async_copy(stats, stats, m_recv.at[who]).wait()
    for k in range(1, dp):
        over_dp(k).start()
    for k in range(1, dp):
        who = lax.rem(me + k, dp)
        pltpu.make_async_copy(slots.at[who], slots.at[who], d_recv.at[who]).wait()
    totals = jnp.sum(slots[...].reshape(dp * mp, *stats.shape), axis=0)
    grad_total = totals[0:1, 0:1]
    pre_total = totals[1:2, 0:1]
    graft = jnp.sqrt(grad_total / jnp.maximum(pre_total, 1.0))
    graft_ref[0, 0] = graft[0, 0]
    out[...] = (pre[...] * graft[None]).astype(jnp.bfloat16)

    def piece(k):
        dest = lax.rem(pair + k, pairs)
        return pltpu.make_async_remote_copy(
            out.at[dest % halves], got.at[pair], u_send.at[k], u_recv.at[pair], (2 * dest + side, col), MESH)

    for k in range(1, pairs):
        piece(k).start()
    got[pair] = out[pair % halves]
    for k in range(1, pairs):
        who = lax.rem(pair + k, pairs)
        pltpu.make_async_copy(got.at[who], got.at[who], u_recv.at[who]).wait()
    for c in range(CB):
        holder = owners[(pair // halves) * CB + c] // 2
        update[:, c * B : (c + 1) * B] = got[holder]
    for k in range(1, mp):
        over_mp(k).wait_send()
    for k in range(1, dp):
        over_dp(k).wait_send()
    for k in range(1, pairs):
        piece(k).wait_send()


def product(left, right):
    return jnp.matmul(left, right, precision=lax.Precision.HIGH, preferred_element_type=jnp.float32)


def inverse_root(stat):
    eye = jnp.eye(B, dtype=jnp.float32)
    size = jnp.sqrt(jnp.sum(stat * stat))
    m = stat / size
    m2 = product(m, m)
    f = (5.0 * eye - m) * 0.25
    f2 = (25.0 * eye - 10.0 * m + m2) * 0.0625
    mf = (5.0 * m - m2) * 0.25
    y = (5.0 * f - product(product(f2, f2), mf)) * 0.25
    my = product(m, y)
    y2 = product(y, y)
    return (5.0 * y - product(product(y2, y2), my)) * (0.25 * size ** (-0.25))


def on_device(activations, cotangents, owners):
    dp = lax.axis_size("dp")
    mp = lax.axis_size("mp")
    me = lax.axis_index("dp")
    pairs = dp // 2
    tokens, features = activations.shape
    part = tokens // mp
    vmem = pl.BlockSpec(memory_space=pltpu.VMEM)
    smem = pl.BlockSpec(memory_space=pltpu.SMEM)
    dma = pltpu.SemaphoreType.DMA
    square = jax.ShapeDtypeStruct((B, B), jnp.float32)
    gradient, oriented = pl.pallas_call(
        functools.partial(gather_kernel, dp, mp),
        out_shape=(square, square),
        in_specs=[smem, vmem, vmem],
        out_specs=(vmem, vmem),
        scratch_shapes=[
            pltpu.VMEM((pairs, part, B), jnp.bfloat16),
            pltpu.VMEM((pairs, tokens, B), jnp.bfloat16),
            pltpu.VMEM((dp, mp, part, B), jnp.bfloat16),
            pltpu.VMEM((dp, tokens, B), jnp.bfloat16),
            dma((pairs,)), dma((pairs,)), dma((dp, mp)), dma((pairs,)), dma((pairs,)), dma((dp, mp)), dma((dp,)),
        ],
        compiler_params=pltpu.CompilerParams(collective_id=0, has_side_effects=True),
    )(owners, activations, cotangents)

    my_left = jnp.any(owners == me)
    grad_total = jnp.sum(oriented * oriented)
    ridge = 0.1 * (grad_total / B + 1.0) * jnp.eye(B, dtype=jnp.float32)
    root = inverse_root(product(oriented, oriented.T) + ridge)

    rows = features // dp
    halves = B // rows // 2

    def my_rows(matrix):
        split = matrix.reshape(halves, 2, rows, B)
        return jnp.where(me % 2 == 0, split[:, 0], split[:, 1]).reshape(halves * rows, B)

    first = jnp.where(my_left, my_rows(root), my_rows(gradient))
    last = jnp.where(my_left, gradient, root)
    pre = product(product(first, root), last)
    row_ids = lax.broadcasted_iota(jnp.int32, (8, 128), 0)
    stats = jnp.where(row_ids == 0, 0.5 * grad_total, jnp.sum(pre * pre))
    update, graft = pl.pallas_call(
        functools.partial(finish_kernel, dp, mp),
        out_shape=(
            jax.ShapeDtypeStruct((rows, CB * B), jnp.bfloat16),
            jax.ShapeDtypeStruct((1, 1), jnp.float32),
        ),
        in_specs=[smem, vmem, vmem],
        out_specs=(vmem, smem),
        scratch_shapes=[
            pltpu.VMEM((dp, mp, 8, 128), jnp.float32),
            pltpu.VMEM((halves, rows, B), jnp.bfloat16),
            pltpu.VMEM((pairs, rows, B), jnp.bfloat16),
            dma((mp,)), dma((mp,)), dma((dp,)), dma((dp,)), dma((pairs,)), dma((pairs,)),
        ],
        compiler_params=pltpu.CompilerParams(collective_id=1, has_side_effects=True),
    )(owners, stats, pre.reshape(halves, rows, B))
    return (update, root, graft[0, 0])


def solution(mesh):
    return jax.shard_map(
        on_device,
        mesh=mesh,
        in_specs=(P("dp", None), P("dp", "mp"), P()),
        out_specs=(P("dp", "mp"), P("dp", "mp"), P()),
        check_vma=False,
    )
```

```python
import functools
import math

import jax
import jax.numpy as jnp
from jax import lax
from jax.experimental import pallas as pl
from jax.experimental.pallas import tpu as pltpu
from jax.sharding import PartitionSpec as P

B = 512
CB = 2
MESH = pl.DeviceIdType.MESH


def split(x):
    high = x.astype(jnp.bfloat16)
    return high, (x - high.astype(jnp.float32)).astype(jnp.bfloat16)


def product(left, right, transposed=False):
    a, b = split(left), split(right)
    axis = 1 if transposed else 0
    return lax.dot_general(
        jnp.concatenate([a[0], a[0], a[1]], axis=1),
        jnp.concatenate([b[0], b[1], b[0]], axis=axis),
        (((1,), (axis,)), ((), ())),
        preferred_element_type=jnp.float32,
    )


def total(x):
    return jnp.sum(jnp.sum(x, axis=0, keepdims=True), axis=1, keepdims=True)


def inverse_root(stat, eye):
    size = jnp.sqrt(total(stat * stat))
    m = stat / size
    m2 = product(m, m)
    f = (5.0 * eye - m) * 0.25
    f2 = (25.0 * eye - 10.0 * m + m2) * 0.0625
    mf = (5.0 * m - m2) * 0.25
    y = (5.0 * f - product(product(f2, f2), mf)) * 0.25
    my = product(m, y)
    y2 = product(y, y)
    return (5.0 * y - product(product(y2, y2), my)) * (0.25 / jnp.sqrt(jnp.sqrt(size)))


def step_kernel(
    dp, mp, owners, acts, cots, update, root, graft_ref, grad, oriented, a_sel, c_sel, a_all, c_all,
    stats, slots, pre, out, got,
    az_send, ax_send, am_send, cz_send, cx_send, a_recv, c_recv, m_send, m_recv, d_send, d_recv, u_send, u_recv,
):
    pairs = dp // 2
    me = lax.axis_index("dp")
    col = lax.axis_index("mp")
    pair = me // 2
    side = me % 2
    across = 2 * pair + 1 - side

    def source(k):
        return 2 * lax.rem(pair + k, pairs) + side

    barrier = pltpu.get_barrier_semaphore()
    for k in range(1, dp):
        pl.semaphore_signal(barrier, inc=1, device_id=(lax.rem(me + k, dp), col), device_id_type=MESH)
    for k in range(1, mp):
        pl.semaphore_signal(barrier, inc=1, device_id=(me, lax.rem(col + k, mp)), device_id_type=MESH)

    def block_of(which):
        held = [jnp.where(owners[b] // 2 == which, b, 0) for b in range(owners.shape[0])]
        return functools.reduce(jnp.add, held)

    def chosen(wide, which):
        parts = [
            wide[:, n * B : (n + 1) * B] * jnp.where(which == n, 1.0, 0.0).astype(wide.dtype)
            for n in range(wide.shape[1] // B)
        ]
        return functools.reduce(jnp.add, parts)

    part = a_sel.shape[1]
    scale = 1.0 / math.sqrt(dp * cots.shape[0])
    for dest in range(pairs):
        block = block_of(dest)
        row_start = pl.multiple_of(col * part, part)
        mine = acts[pl.ds(row_start, part), :]
        a_sel[dest] = chosen(mine, block // CB)
        c_sel[dest] = chosen(cots[...], block % CB)
    is_left = functools.reduce(
        jnp.add, [jnp.where(owners[b] == me, 1.0, 0.0) for b in range(owners.shape[0])])
    a_all[me, col] = a_sel[pair]
    c_all[me] = c_sel[pair]
    pl.semaphore_wait(barrier, dp - 1 + mp - 1)

    def a_pair(k):
        dest = lax.rem(pair + k, pairs)
        return pltpu.make_async_remote_copy(
            a_sel.at[dest], a_all.at[me, col], az_send.at[k], a_recv.at[me, col], (source(k), col), MESH)

    def c_pair(k):
        dest = lax.rem(pair + k, pairs)
        return pltpu.make_async_remote_copy(
            c_sel.at[dest], c_all.at[me], cz_send.at[k], c_recv.at[me], (source(k), col), MESH)

    def a_across(k):
        src = source(k)
        ref = a_sel.at[pair] if k == 0 else a_all.at[src, col]
        return pltpu.make_async_remote_copy(
            ref, a_all.at[src, col], ax_send.at[k], a_recv.at[src, col], (across, col), MESH)

    def c_across(k):
        src = source(k)
        ref = c_sel.at[pair] if k == 0 else c_all.at[src]
        return pltpu.make_async_remote_copy(
            ref, c_all.at[src], cx_send.at[k], c_recv.at[src], (across, col), MESH)

    def a_mp(src, k, own=False):
        ref = a_sel.at[pair] if own else a_all.at[src, col]
        return pltpu.make_async_remote_copy(
            ref, a_all.at[src, col], am_send.at[src, k], a_recv.at[src, col], (me, lax.rem(col + k, mp)), MESH)

    def start_mp(src):
        @pl.loop(1, mp)
        def _(k):
            a_mp(src, k).start()

    def a_arrived(src, who):
        pltpu.make_async_copy(a_all.at[src, who], a_all.at[src, who], a_recv.at[src, who]).wait()

    def c_arrived(src):
        pltpu.make_async_copy(c_all.at[src], c_all.at[src], c_recv.at[src]).wait()

    order = list(range(1, pairs))
    a_across(0).start()
    for k in order:
        a_pair(k).start()
    c_across(0).start()
    for k in order:
        c_pair(k).start()

    @pl.loop(1, mp)
    def _(k):
        a_mp(me, k, own=True).start()

    for k in order:
        a_arrived(source(k), col)
        a_across(k).start()
        start_mp(source(k))
    for k in range(pairs):
        other = source(k) + 1 - 2 * side
        a_arrived(other, col)
        start_mp(other)
    def a_complete(src):
        @pl.loop(1, mp)
        def _(k):
            a_arrived(src, lax.rem(col + k, mp))

    def accumulate(k):
        base = 2 * lax.rem(pair + k, pairs)
        a_complete(base)
        a_complete(base + 1)
        c_arrived(source(k) + 1 - 2 * side)
        tokens = 2 * cots.shape[0]
        a = a_all[pl.ds(base, 2)].reshape(tokens, B)
        c = c_all[pl.ds(base, 2)].reshape(tokens, B)
        keep = is_left.astype(a.dtype)
        swap = (1.0 - is_left).astype(a.dtype)
        first = a * keep + c * swap
        second = c * keep + a * swap
        dims = (((0,), (0,)), ((), ()))
        add = lax.dot_general(a, c, dims, preferred_element_type=jnp.float32) * scale
        add_oriented = lax.dot_general(first, second, dims, preferred_element_type=jnp.float32) * scale
        if k == 0:
            grad[...] = add
            oriented[...] = add_oriented
        else:
            grad[...] += add
            oriented[...] += add_oriented

    for k in order:
        c_arrived(source(k))
        c_across(k).start()
        accumulate(k - 1)
    accumulate(pairs - 1)

    g = oriented[...]
    grad_total = total(g * g)
    ids = lax.broadcasted_iota(jnp.int32, (B, B), 0), lax.broadcasted_iota(jnp.int32, (B, B), 1)
    eye = jnp.where(ids[0] == ids[1], 1.0, 0.0)
    ridge = 0.1 * (grad_total / B + 1.0)
    root[...] = inverse_root(product(g, g, transposed=True) + ridge * eye, eye)
    is_right = 1.0 - is_left
    halves, rows = out.shape[:2]
    starts = [pl.multiple_of((2 * h + side) * rows, rows) for h in range(halves)]
    first = jnp.concatenate(
        [root[pl.ds(n, rows), :] * is_left + grad[pl.ds(n, rows), :] * is_right for n in starts], axis=0)
    last = grad[...] * is_left + root[...] * is_right
    mine = product(product(first, root[...]), last)
    row_ids = lax.broadcasted_iota(jnp.int32, stats.shape, 0)
    stats[...] = jnp.where(row_ids == 0, 0.5 * grad_total, total(mine * mine))
    slots[me, col] = stats[...]
    pre[...] = mine.reshape(halves, rows, B)

    def over_mp(k):
        return pltpu.make_async_remote_copy(
            stats, slots.at[me, col], m_send.at[k], m_recv.at[col], (me, lax.rem(col + k, mp)), MESH)

    def over_dp(k):
        return pltpu.make_async_remote_copy(
            slots.at[me], slots.at[me], d_send.at[k], d_recv.at[me], (lax.rem(me + k, dp), col), MESH)

    for k in range(1, mp):
        over_mp(k).start()
    for k in range(1, mp):
        who = lax.rem(col + k, mp)
        pltpu.make_async_copy(stats, stats, m_recv.at[who]).wait()
    for k in range(1, dp):
        over_dp(k).start()
    for k in range(1, dp):
        who = lax.rem(me + k, dp)
        pltpu.make_async_copy(slots.at[who], slots.at[who], d_recv.at[who]).wait()
    totals = jnp.sum(slots[...].reshape(dp * mp, *stats.shape), axis=0)
    grad_total = totals[0:1, 0:1]
    pre_total = totals[1:2, 0:1]
    graft = jnp.sqrt(grad_total / jnp.maximum(pre_total, 1.0))
    graft_ref[0, 0] = graft[0, 0]
    out[...] = (pre[...] * graft[None]).astype(jnp.bfloat16)

    def piece(k):
        dest = lax.rem(pair + k, pairs)
        return pltpu.make_async_remote_copy(
            out.at[dest % halves], got.at[pair], u_send.at[k], u_recv.at[pair], (2 * dest + side, col), MESH)

    for k in range(1, pairs):
        piece(k).start()
    got[pair] = out[pair % halves]
    for k in range(1, pairs):
        who = lax.rem(pair + k, pairs)
        pltpu.make_async_copy(got.at[who], got.at[who], u_recv.at[who]).wait()
    for c in range(CB):
        holder = owners[(pair // halves) * CB + c] // 2
        update[:, c * B : (c + 1) * B] = got[holder]
    @pl.loop(0, dp)
    def _(src):
        @pl.loop(1, mp)
        def _(k):
            a_mp(src, k).wait_send()

    for k in range(pairs):
        a_across(k).wait_send()
        c_across(k).wait_send()
    for k in order:
        a_pair(k).wait_send()
        c_pair(k).wait_send()
    for k in range(1, mp):
        over_mp(k).wait_send()
    for k in range(1, dp):
        over_dp(k).wait_send()
    for k in range(1, pairs):
        piece(k).wait_send()


def on_device(activations, cotangents, owners):
    dp = lax.axis_size("dp")
    mp = lax.axis_size("mp")
    pairs = dp // 2
    tokens, features = activations.shape
    part = tokens // mp
    rows = features // dp
    halves = B // rows // 2
    vmem = pl.BlockSpec(memory_space=pltpu.VMEM)
    smem = pl.BlockSpec(memory_space=pltpu.SMEM)
    dma = pltpu.SemaphoreType.DMA
    update, root, graft = pl.pallas_call(
        functools.partial(step_kernel, dp, mp),
        out_shape=(
            jax.ShapeDtypeStruct((rows, CB * B), jnp.bfloat16),
            jax.ShapeDtypeStruct((B, B), jnp.float32),
            jax.ShapeDtypeStruct((1, 1), jnp.float32),
        ),
        in_specs=[smem, vmem, vmem],
        out_specs=(vmem, vmem, smem),
        scratch_shapes=[
            pltpu.VMEM((B, B), jnp.float32),
            pltpu.VMEM((B, B), jnp.float32),
            pltpu.VMEM((pairs, part, B), jnp.bfloat16),
            pltpu.VMEM((pairs, tokens, B), jnp.bfloat16),
            pltpu.VMEM((dp, mp, part, B), jnp.bfloat16),
            pltpu.VMEM((dp, tokens, B), jnp.bfloat16),
            pltpu.VMEM((8, 128), jnp.float32),
            pltpu.VMEM((dp, mp, 8, 128), jnp.float32),
            pltpu.VMEM((halves, rows, B), jnp.float32),
            pltpu.VMEM((halves, rows, B), jnp.bfloat16),
            pltpu.VMEM((pairs, rows, B), jnp.bfloat16),
            dma((pairs,)), dma((pairs,)), dma((dp, mp)), dma((pairs,)), dma((pairs,)), dma((dp, mp)), dma((dp,)),
            dma((mp,)), dma((mp,)), dma((dp,)), dma((dp,)), dma((pairs,)), dma((pairs,)),
        ],
        compiler_params=pltpu.CompilerParams(collective_id=0, has_side_effects=True),
    )(owners, activations, cotangents)
    return (update, root, graft[0, 0])


def solution(mesh):
    return jax.shard_map(
        on_device,
        mesh=mesh,
        in_specs=(P("dp", None), P("dp", "mp"), P()),
        out_specs=(P("dp", "mp"), P("dp", "mp"), P()),
        check_vma=False,
    )
```

```python
import functools
import math

import jax
import jax.numpy as jnp
from jax import lax
from jax.experimental import pallas as pl
from jax.experimental.pallas import tpu as pltpu
from jax.sharding import PartitionSpec as P

B = 512
CB = 2
CHUNKS = 2
MESH = pl.DeviceIdType.MESH


def split(x):
    high = x.astype(jnp.bfloat16)
    return high, (x - high.astype(jnp.float32)).astype(jnp.bfloat16)


def product(left, right, transposed=False):
    a, b = split(left), split(right)
    axis = 1 if transposed else 0
    return lax.dot_general(
        jnp.concatenate([a[0], a[0], a[1]], axis=1),
        jnp.concatenate([b[0], b[1], b[0]], axis=axis),
        (((1,), (axis,)), ((), ())),
        preferred_element_type=jnp.float32,
    )


def total(x):
    return jnp.sum(jnp.sum(x, axis=0, keepdims=True), axis=1, keepdims=True)


def inverse_root(stat, eye):
    size = jnp.sqrt(total(stat * stat))
    m = stat / size
    m2 = product(m, m)
    f = (5.0 * eye - m) * 0.25
    f2 = (25.0 * eye - 10.0 * m + m2) * 0.0625
    mf = (5.0 * m - m2) * 0.25
    y = (5.0 * f - product(product(f2, f2), mf)) * 0.25
    my = product(m, y)
    y2 = product(y, y)
    return (5.0 * y - product(product(y2, y2), my)) * 0.25, 1.0 / jnp.sqrt(jnp.sqrt(size))


def step_kernel(
    dp, mp, owners, acts_in, cots_in, update, root, scale_ref, graft_ref, acts, cots, in_sem, grad, oriented, a_sel, c_sel, a_all, c_all,
    stats, slots, pre, out, got,
    az_send, ax_send, am_send, cz_send, cx_send, a_recv, c_recv, m_send, m_recv, d_send, d_recv, u_send, u_recv,
):
    pairs = dp // 2
    me = lax.axis_index("dp")
    col = lax.axis_index("mp")
    pair = me // 2
    side = me % 2
    across = 2 * pair + 1 - side

    def source(k):
        return 2 * lax.rem(pair + k, pairs) + side

    barrier = pltpu.get_barrier_semaphore()
    for k in range(1, dp):
        pl.semaphore_signal(barrier, inc=1, device_id=(lax.rem(me + k, dp), col), device_id_type=MESH)
    for k in range(1, mp):
        pl.semaphore_signal(barrier, inc=1, device_id=(me, lax.rem(col + k, mp)), device_id_type=MESH)

    fetches = [
        pltpu.make_async_copy(acts_in, acts, in_sem.at[0]),
        pltpu.make_async_copy(cots_in, cots, in_sem.at[1]),
    ]
    for fetch in fetches:
        fetch.start()
    for fetch in fetches:
        fetch.wait()

    def block_of(which):
        held = [jnp.where(owners[b] // 2 == which, b, 0) for b in range(owners.shape[0])]
        return functools.reduce(jnp.add, held)

    def chosen(wide, which):
        parts = [
            wide[:, n * B : (n + 1) * B] * jnp.where(which == n, 1.0, 0.0).astype(wide.dtype)
            for n in range(wide.shape[1] // B)
        ]
        return functools.reduce(jnp.add, parts)

    part = a_sel.shape[1]
    scale = 1.0 / math.sqrt(dp * cots.shape[0])
    for dest in range(pairs):
        block = block_of(dest)
        row_start = pl.multiple_of(col * part, part)
        mine = acts[pl.ds(row_start, part), :]
        a_sel[dest] = chosen(mine, block // CB)
        c_sel[dest] = chosen(cots[...], block % CB)
    is_left = functools.reduce(
        jnp.add, [jnp.where(owners[b] == me, 1.0, 0.0) for b in range(owners.shape[0])])
    a_all[me, col] = a_sel[pair]
    c_all[me] = c_sel[pair]
    pl.semaphore_wait(barrier, dp - 1 + mp - 1)

    def a_pair(k):
        dest = lax.rem(pair + k, pairs)
        return pltpu.make_async_remote_copy(
            a_sel.at[dest], a_all.at[me, col], az_send.at[k], a_recv.at[me, col], (source(k), col), MESH)

    chunk = cots.shape[0] // CHUNKS

    def c_pair(k, h):
        dest = lax.rem(pair + k, pairs)
        cut = pl.ds(h * chunk, chunk)
        return pltpu.make_async_remote_copy(
            c_sel.at[dest, cut], c_all.at[me, cut], cz_send.at[k, h], c_recv.at[me, h], (source(k), col), MESH)

    def a_across(k):
        src = source(k)
        ref = a_sel.at[pair] if k == 0 else a_all.at[src, col]
        return pltpu.make_async_remote_copy(
            ref, a_all.at[src, col], ax_send.at[k], a_recv.at[src, col], (across, col), MESH)

    def c_across(k, h):
        src = source(k)
        cut = pl.ds(h * chunk, chunk)
        ref = c_sel.at[pair, cut] if k == 0 else c_all.at[src, cut]
        return pltpu.make_async_remote_copy(
            ref, c_all.at[src, cut], cx_send.at[k, h], c_recv.at[src, h], (across, col), MESH)

    def a_mp(src, k, own=False):
        ref = a_sel.at[pair] if own else a_all.at[src, col]
        return pltpu.make_async_remote_copy(
            ref, a_all.at[src, col], am_send.at[src, k], a_recv.at[src, col], (me, lax.rem(col + k, mp)), MESH)

    def start_mp(src):
        @pl.loop(1, mp)
        def _(k):
            a_mp(src, k).start()

    def a_arrived(src, who):
        pltpu.make_async_copy(a_all.at[src, who], a_all.at[src, who], a_recv.at[src, who]).wait()

    def c_arrived(src, h):
        ref = c_all.at[src, pl.ds(h * chunk, chunk)]
        pltpu.make_async_copy(ref, ref, c_recv.at[src, h]).wait()

    order = list(range(1, pairs))
    a_across(0).start()
    for k in order:
        a_pair(k).start()
    for h in range(CHUNKS):
        c_across(0, h).start()
        for k in order:
            c_pair(k, h).start()

    @pl.loop(1, mp)
    def _(k):
        a_mp(me, k, own=True).start()

    for k in order:
        a_arrived(source(k), col)
        a_across(k).start()
        start_mp(source(k))
    for k in range(pairs):
        other = source(k) + 1 - 2 * side
        a_arrived(other, col)
        start_mp(other)
    def a_complete(src):
        @pl.loop(1, mp)
        def _(k):
            a_arrived(src, lax.rem(col + k, mp))

    def accumulate(k):
        base = 2 * lax.rem(pair + k, pairs)
        a_complete(base)
        a_complete(base + 1)
        for h in range(CHUNKS):
            c_arrived(source(k) + 1 - 2 * side, h)
        tokens = 2 * cots.shape[0]
        a = a_all[pl.ds(base, 2)].reshape(tokens, B)
        c = c_all[pl.ds(base, 2)].reshape(tokens, B)
        keep = is_left.astype(a.dtype)
        swap = (1.0 - is_left).astype(a.dtype)
        first = a * keep + c * swap
        second = c * keep + a * swap
        dims = (((0,), (0,)), ((), ()))
        add = lax.dot_general(a, c, dims, preferred_element_type=jnp.float32) * scale
        add_oriented = lax.dot_general(first, second, dims, preferred_element_type=jnp.float32) * scale
        if k == 0:
            grad[...] = add
            oriented[...] = add_oriented
        else:
            grad[...] += add
            oriented[...] += add_oriented

    for h in range(CHUNKS):
        for k in order:
            c_arrived(source(k), h)
            c_across(k, h).start()
            if h == CHUNKS - 1:
                accumulate(k - 1)
    accumulate(pairs - 1)

    g = oriented[...]
    grad_total = total(g * g)
    ids = lax.broadcasted_iota(jnp.int32, (B, B), 0), lax.broadcasted_iota(jnp.int32, (B, B), 1)
    eye = jnp.where(ids[0] == ids[1], 1.0, 0.0)
    ridge = 0.1 * (grad_total / B + 1.0)
    root[...], factor = inverse_root(product(g, g, transposed=True) + ridge * eye, eye)
    scale_ref[0, 0] = factor[0, 0]
    is_right = 1.0 - is_left
    halves, rows = out.shape[:2]
    starts = [pl.multiple_of((2 * h + side) * rows, rows) for h in range(halves)]
    first = jnp.concatenate(
        [root[pl.ds(n, rows), :] * is_left + grad[pl.ds(n, rows), :] * is_right for n in starts], axis=0)
    last = grad[...] * is_left + root[...] * is_right
    mine = product(product(first, root[...]), last) * (factor * factor)
    row_ids = lax.broadcasted_iota(jnp.int32, stats.shape, 0)
    stats[...] = jnp.where(row_ids == 0, 0.5 * grad_total, total(mine * mine))
    slots[me, col] = stats[...]
    pre[...] = mine.reshape(halves, rows, B)

    def over_mp(k):
        return pltpu.make_async_remote_copy(
            stats, slots.at[me, col], m_send.at[k], m_recv.at[col], (me, lax.rem(col + k, mp)), MESH)

    def over_dp(k):
        return pltpu.make_async_remote_copy(
            slots.at[me], slots.at[me], d_send.at[k], d_recv.at[me], (lax.rem(me + k, dp), col), MESH)

    for k in range(1, mp):
        over_mp(k).start()
    for k in range(1, mp):
        who = lax.rem(col + k, mp)
        pltpu.make_async_copy(stats, stats, m_recv.at[who]).wait()
    for k in range(1, dp):
        over_dp(k).start()
    for k in range(1, dp):
        who = lax.rem(me + k, dp)
        pltpu.make_async_copy(slots.at[who], slots.at[who], d_recv.at[who]).wait()
    totals = jnp.sum(slots[...].reshape(dp * mp, *stats.shape), axis=0)
    grad_total = totals[0:1, 0:1]
    pre_total = totals[1:2, 0:1]
    graft = jnp.sqrt(grad_total / jnp.maximum(pre_total, 1.0))
    graft_ref[0, 0] = graft[0, 0]
    out[...] = (pre[...] * graft[None]).astype(jnp.bfloat16)

    def piece(k):
        dest = lax.rem(pair + k, pairs)
        return pltpu.make_async_remote_copy(
            out.at[dest % halves], got.at[pair], u_send.at[k], u_recv.at[pair], (2 * dest + side, col), MESH)

    for k in range(1, pairs):
        piece(k).start()
    got[pair] = out[pair % halves]
    for k in range(1, pairs):
        who = lax.rem(pair + k, pairs)
        pltpu.make_async_copy(got.at[who], got.at[who], u_recv.at[who]).wait()
    for c in range(CB):
        holder = owners[(pair // halves) * CB + c] // 2
        update[c] = got[holder]
    @pl.loop(0, dp)
    def _(src):
        @pl.loop(1, mp)
        def _(k):
            a_mp(src, k).wait_send()

    for k in range(pairs):
        a_across(k).wait_send()
        for h in range(CHUNKS):
            c_across(k, h).wait_send()
    for k in order:
        a_pair(k).wait_send()
        for h in range(CHUNKS):
            c_pair(k, h).wait_send()
    for k in range(1, mp):
        over_mp(k).wait_send()
    for k in range(1, dp):
        over_dp(k).wait_send()
    for k in range(1, pairs):
        piece(k).wait_send()


def on_device(activations, cotangents, owners):
    dp = lax.axis_size("dp")
    mp = lax.axis_size("mp")
    pairs = dp // 2
    tokens, features = activations.shape
    part = tokens // mp
    rows = features // dp
    halves = B // rows // 2
    vmem = pl.BlockSpec(memory_space=pltpu.VMEM)
    smem = pl.BlockSpec(memory_space=pltpu.SMEM)
    anywhere = pl.BlockSpec(memory_space=pl.ANY)
    dma = pltpu.SemaphoreType.DMA
    update, root, scale, graft = pl.pallas_call(
        functools.partial(step_kernel, dp, mp),
        out_shape=(
            jax.ShapeDtypeStruct((CB, rows, B), jnp.bfloat16),
            jax.ShapeDtypeStruct((B, B), jnp.float32),
            jax.ShapeDtypeStruct((1, 1), jnp.float32),
            jax.ShapeDtypeStruct((1, 1), jnp.float32),
        ),
        in_specs=[smem, anywhere, anywhere],
        out_specs=(vmem, vmem, smem, smem),
        scratch_shapes=[
            pltpu.VMEM(activations.shape, jnp.bfloat16),
            pltpu.VMEM(cotangents.shape, jnp.bfloat16),
            dma((2,)),
            pltpu.VMEM((B, B), jnp.float32),
            pltpu.VMEM((B, B), jnp.float32),
            pltpu.VMEM((pairs, part, B), jnp.bfloat16),
            pltpu.VMEM((pairs, tokens, B), jnp.bfloat16),
            pltpu.VMEM((dp, mp, part, B), jnp.bfloat16),
            pltpu.VMEM((dp, tokens, B), jnp.bfloat16),
            pltpu.VMEM((8, 128), jnp.float32),
            pltpu.VMEM((dp, mp, 8, 128), jnp.float32),
            pltpu.VMEM((halves, rows, B), jnp.float32),
            pltpu.VMEM((halves, rows, B), jnp.bfloat16),
            pltpu.VMEM((pairs, rows, B), jnp.bfloat16),
            dma((pairs,)), dma((pairs,)), dma((dp, mp)), dma((pairs, CHUNKS)), dma((pairs, CHUNKS)), dma((dp, mp)), dma((dp, CHUNKS)),
            dma((mp,)), dma((mp,)), dma((dp,)), dma((dp,)), dma((pairs,)), dma((pairs,)),
        ],
        compiler_params=pltpu.CompilerParams(collective_id=0, has_side_effects=True),
    )(owners, activations, cotangents)
    return (jnp.concatenate([update[c] for c in range(CB)], axis=1), root * scale, graft[0, 0])


def solution(mesh):
    return jax.shard_map(
        on_device,
        mesh=mesh,
        in_specs=(P("dp", None), P("dp", "mp"), P()),
        out_specs=(P("dp", "mp"), P("dp", "mp"), P()),
        check_vma=False,
    )
```

```python
import functools
import math

import jax
import jax.numpy as jnp
from jax import lax
from jax.experimental import pallas as pl
from jax.experimental.pallas import tpu as pltpu
from jax.sharding import PartitionSpec as P

B = 512
CB = 2
CHUNKS = 2
MESH = pl.DeviceIdType.MESH


def split(x):
    high = x.astype(jnp.bfloat16)
    return high, (x - high.astype(jnp.float32)).astype(jnp.bfloat16)


def product(left, right, transposed=False):
    a, b = split(left), split(right)
    axis = 1 if transposed else 0
    return lax.dot_general(
        jnp.concatenate([a[0], a[0], a[1]], axis=1),
        jnp.concatenate([b[0], b[1], b[0]], axis=axis),
        (((1,), (axis,)), ((), ())),
        preferred_element_type=jnp.float32,
    )


def total(x):
    return jnp.sum(jnp.sum(x, axis=0, keepdims=True), axis=1, keepdims=True)


def inverse_root(stat, eye):
    size = jnp.sqrt(total(stat * stat))
    m = stat / size
    m2 = product(m, m)
    f = (5.0 * eye - m) * 0.25
    f2 = (25.0 * eye - 10.0 * m + m2) * 0.0625
    mf = (5.0 * m - m2) * 0.25
    y = (5.0 * f - product(product(f2, f2), mf)) * 0.25
    my = product(m, y)
    y2 = product(y, y)
    return (5.0 * y - product(product(y2, y2), my)) * 0.25, 1.0 / jnp.sqrt(jnp.sqrt(size))


def step_kernel(
    dp, mp, owners, acts, cots, update, root, scale_ref, graft_ref, grad, oriented, a_sel, c_sel, a_all, c_all,
    stats, slots, pre, out, got,
    az_send, ax_send, am_send, cz_send, cx_send, a_recv, c_recv, d_send, d_recv, u_send, u_recv,
):
    pairs = dp // 2
    me = lax.axis_index("dp")
    col = lax.axis_index("mp")
    pair = me // 2
    side = me % 2
    across = 2 * pair + 1 - side

    def source(k):
        return 2 * lax.rem(pair + k, pairs) + side

    barrier = pltpu.get_barrier_semaphore()
    count = dp * mp
    flat = me * mp + col

    def peer(k):
        other = lax.rem(flat + k, count)
        return other // mp, lax.rem(other, mp)

    @pl.loop(1, count)
    def _(k):
        pl.semaphore_signal(barrier, inc=1, device_id=peer(k), device_id_type=MESH)


    def block_of(which):
        held = [jnp.where(owners[b] // 2 == which, b, 0) for b in range(owners.shape[0])]
        return functools.reduce(jnp.add, held)

    def chosen(wide, which):
        parts = [
            wide[:, n * B : (n + 1) * B] * jnp.where(which == n, 1.0, 0.0).astype(wide.dtype)
            for n in range(wide.shape[1] // B)
        ]
        return functools.reduce(jnp.add, parts)

    part = a_sel.shape[1]
    scale = 1.0 / math.sqrt(dp * cots.shape[0])
    for dest in range(pairs):
        block = block_of(dest)
        row_start = pl.multiple_of(col * part, part)
        mine = acts[pl.ds(row_start, part), :]
        a_sel[dest] = chosen(mine, block // CB)
        c_sel[dest] = chosen(cots[...], block % CB)
    is_left = functools.reduce(
        jnp.add, [jnp.where(owners[b] == me, 1.0, 0.0) for b in range(owners.shape[0])])
    a_all[me, col] = a_sel[pair]
    c_all[me] = c_sel[pair]
    pl.semaphore_wait(barrier, count - 1)

    def a_pair(k):
        dest = lax.rem(pair + k, pairs)
        return pltpu.make_async_remote_copy(
            a_sel.at[dest], a_all.at[me, col], az_send.at[k], a_recv.at[me, col], (source(k), col), MESH)

    chunk = cots.shape[0] // CHUNKS

    def c_pair(k, h):
        dest = lax.rem(pair + k, pairs)
        cut = pl.ds(h * chunk, chunk)
        return pltpu.make_async_remote_copy(
            c_sel.at[dest, cut], c_all.at[me, cut], cz_send.at[k, h], c_recv.at[me, h], (source(k), col), MESH)

    def a_across(k):
        src = source(k)
        ref = a_sel.at[pair] if k == 0 else a_all.at[src, col]
        return pltpu.make_async_remote_copy(
            ref, a_all.at[src, col], ax_send.at[k], a_recv.at[src, col], (across, col), MESH)

    def c_across(k, h):
        src = source(k)
        cut = pl.ds(h * chunk, chunk)
        ref = c_sel.at[pair, cut] if k == 0 else c_all.at[src, cut]
        return pltpu.make_async_remote_copy(
            ref, c_all.at[src, cut], cx_send.at[k, h], c_recv.at[src, h], (across, col), MESH)

    def a_mp(src, k, own=False):
        ref = a_sel.at[pair] if own else a_all.at[src, col]
        return pltpu.make_async_remote_copy(
            ref, a_all.at[src, col], am_send.at[src, k], a_recv.at[src, col], (me, lax.rem(col + k, mp)), MESH)

    def start_mp(src):
        @pl.loop(1, mp)
        def _(k):
            a_mp(src, k).start()

    def a_arrived(src, who):
        pltpu.make_async_copy(a_all.at[src, who], a_all.at[src, who], a_recv.at[src, who]).wait()

    def c_arrived(src, h):
        ref = c_all.at[src, pl.ds(h * chunk, chunk)]
        pltpu.make_async_copy(ref, ref, c_recv.at[src, h]).wait()

    order = list(range(1, pairs))
    a_across(0).start()
    for k in order:
        a_pair(k).start()
    for h in range(CHUNKS):
        c_across(0, h).start()
        for k in order:
            c_pair(k, h).start()

    @pl.loop(1, mp)
    def _(k):
        a_mp(me, k, own=True).start()

    for k in order:
        a_arrived(source(k), col)
        a_across(k).start()
        start_mp(source(k))
    for k in range(pairs):
        other = source(k) + 1 - 2 * side
        a_arrived(other, col)
        start_mp(other)
    def a_complete(src):
        @pl.loop(1, mp)
        def _(k):
            a_arrived(src, lax.rem(col + k, mp))

    def accumulate(k):
        base = 2 * lax.rem(pair + k, pairs)
        a_complete(base)
        a_complete(base + 1)
        for h in range(CHUNKS):
            c_arrived(source(k) + 1 - 2 * side, h)
        tokens = 2 * cots.shape[0]
        a = a_all[pl.ds(base, 2)].reshape(tokens, B)
        c = c_all[pl.ds(base, 2)].reshape(tokens, B)
        keep = is_left.astype(a.dtype)
        swap = (1.0 - is_left).astype(a.dtype)
        first = a * keep + c * swap
        second = c * keep + a * swap
        dims = (((0,), (0,)), ((), ()))
        add = lax.dot_general(a, c, dims, preferred_element_type=jnp.float32) * scale
        add_oriented = lax.dot_general(first, second, dims, preferred_element_type=jnp.float32) * scale
        if k == 0:
            grad[...] = add
            oriented[...] = add_oriented
        else:
            grad[...] += add
            oriented[...] += add_oriented

    for h in range(CHUNKS):
        for k in order:
            c_arrived(source(k), h)
            c_across(k, h).start()
            if h == CHUNKS - 1:
                accumulate(k - 1)
    accumulate(pairs - 1)

    g = oriented[...]
    grad_total = total(g * g)
    ids = lax.broadcasted_iota(jnp.int32, (B, B), 0), lax.broadcasted_iota(jnp.int32, (B, B), 1)
    eye = jnp.where(ids[0] == ids[1], 1.0, 0.0)
    ridge = 0.1 * (grad_total / B + 1.0)
    root[...], factor = inverse_root(product(g, g, transposed=True) + ridge * eye, eye)
    scale_ref[0, 0] = factor[0, 0]
    is_right = 1.0 - is_left
    halves, rows = out.shape[:2]
    starts = [pl.multiple_of((2 * h + side) * rows, rows) for h in range(halves)]
    first = jnp.concatenate(
        [root[pl.ds(n, rows), :] * is_left + grad[pl.ds(n, rows), :] * is_right for n in starts], axis=0)
    last = grad[...] * is_left + root[...] * is_right
    mine = product(product(first, root[...]), last) * (factor * factor)
    row_ids = lax.broadcasted_iota(jnp.int32, stats.shape, 0)
    stats[...] = jnp.where(row_ids == 0, 0.5 * grad_total, total(mine * mine))
    slots[me, col] = stats[...]
    pre[...] = mine.reshape(halves, rows, B)

    def share(k):
        return pltpu.make_async_remote_copy(
            stats, slots.at[me, col], d_send.at[k], d_recv.at[flat], peer(k), MESH)

    @pl.loop(1, count)
    def _(k):
        share(k).start()

    @pl.loop(1, count)
    def _(k):
        pltpu.make_async_copy(stats, stats, d_recv.at[lax.rem(flat + k, count)]).wait()

    totals = jnp.sum(slots[...].reshape(dp * mp, *stats.shape), axis=0)
    grad_total = totals[0:1, 0:1]
    pre_total = totals[1:2, 0:1]
    graft = jnp.sqrt(grad_total / jnp.maximum(pre_total, 1.0))
    graft_ref[0, 0] = graft[0, 0]
    out[...] = (pre[...] * graft[None]).astype(jnp.bfloat16)

    def piece(k):
        dest = lax.rem(pair + k, pairs)
        return pltpu.make_async_remote_copy(
            out.at[dest % halves], got.at[pair], u_send.at[k], u_recv.at[pair], (2 * dest + side, col), MESH)

    for k in range(1, pairs):
        piece(k).start()
    got[pair] = out[pair % halves]
    for k in range(1, pairs):
        who = lax.rem(pair + k, pairs)
        pltpu.make_async_copy(got.at[who], got.at[who], u_recv.at[who]).wait()
    for c in range(CB):
        holder = owners[(pair // halves) * CB + c] // 2
        update[:, c * B : (c + 1) * B] = got[holder]
    @pl.loop(0, dp)
    def _(src):
        @pl.loop(1, mp)
        def _(k):
            a_mp(src, k).wait_send()

    for k in range(pairs):
        a_across(k).wait_send()
        for h in range(CHUNKS):
            c_across(k, h).wait_send()
    for k in order:
        a_pair(k).wait_send()
        for h in range(CHUNKS):
            c_pair(k, h).wait_send()

    @pl.loop(1, count)
    def _(k):
        share(k).wait_send()

    for k in range(1, pairs):
        piece(k).wait_send()


def on_device(activations, cotangents, owners):
    dp = lax.axis_size("dp")
    mp = lax.axis_size("mp")
    pairs = dp // 2
    tokens, features = activations.shape
    part = tokens // mp
    rows = features // dp
    halves = B // rows // 2
    vmem = pl.BlockSpec(memory_space=pltpu.VMEM)
    smem = pl.BlockSpec(memory_space=pltpu.SMEM)
    dma = pltpu.SemaphoreType.DMA
    update, root, scale, graft = pl.pallas_call(
        functools.partial(step_kernel, dp, mp),
        out_shape=(
            jax.ShapeDtypeStruct((rows, CB * B), jnp.bfloat16),
            jax.ShapeDtypeStruct((B, B), jnp.float32),
            jax.ShapeDtypeStruct((1, 1), jnp.float32),
            jax.ShapeDtypeStruct((1, 1), jnp.float32),
        ),
        in_specs=[smem, vmem, vmem],
        out_specs=(vmem, vmem, smem, smem),
        scratch_shapes=[
            pltpu.VMEM((B, B), jnp.float32),
            pltpu.VMEM((B, B), jnp.float32),
            pltpu.VMEM((pairs, part, B), jnp.bfloat16),
            pltpu.VMEM((pairs, tokens, B), jnp.bfloat16),
            pltpu.VMEM((dp, mp, part, B), jnp.bfloat16),
            pltpu.VMEM((dp, tokens, B), jnp.bfloat16),
            pltpu.VMEM((8, 128), jnp.float32),
            pltpu.VMEM((dp, mp, 8, 128), jnp.float32),
            pltpu.VMEM((halves, rows, B), jnp.float32),
            pltpu.VMEM((halves, rows, B), jnp.bfloat16),
            pltpu.VMEM((pairs, rows, B), jnp.bfloat16),
            dma((pairs,)), dma((pairs,)), dma((dp, mp)), dma((pairs, CHUNKS)), dma((pairs, CHUNKS)), dma((dp, mp)), dma((dp, CHUNKS)),
            dma((dp * mp,)), dma((dp * mp,)), dma((pairs,)), dma((pairs,)),
        ],
        compiler_params=pltpu.CompilerParams(collective_id=0, has_side_effects=True, vmem_limit_bytes=48 * 1024 * 1024),
    )(owners, activations, cotangents)
    return (update, root * scale, graft[0, 0])


def solution(mesh):
    return jax.shard_map(
        on_device,
        mesh=mesh,
        in_specs=(P("dp", None), P("dp", "mp"), P()),
        out_specs=(P("dp", "mp"), P("dp", "mp"), P()),
        check_vma=False,
    )
```

```python
import functools
import math

import jax
import jax.numpy as jnp
from jax import lax
from jax.experimental import pallas as pl
from jax.experimental.pallas import tpu as pltpu
from jax.sharding import PartitionSpec as P

B = 512
CB = 2
CHUNKS = 2
MESH = pl.DeviceIdType.MESH


def split(x):
    high = x.astype(jnp.bfloat16)
    return high, (x - high.astype(jnp.float32)).astype(jnp.bfloat16)


def product(left, right, transposed=False):
    a, b = split(left), split(right)
    axis = 1 if transposed else 0
    return lax.dot_general(
        jnp.concatenate([a[0], a[0], a[1]], axis=1),
        jnp.concatenate([b[0], b[1], b[0]], axis=axis),
        (((1,), (axis,)), ((), ())),
        preferred_element_type=jnp.float32,
    )


def total(x):
    return jnp.sum(jnp.sum(x, axis=0, keepdims=True), axis=1, keepdims=True)


def inverse_root(stat, eye):
    size = jnp.sqrt(total(stat * stat))
    m = stat / size
    m2 = product(m, m)
    f = (5.0 * eye - m) * 0.25
    f2 = (25.0 * eye - 10.0 * m + m2) * 0.0625
    mf = (5.0 * m - m2) * 0.25
    y = (5.0 * f - product(product(f2, f2), mf)) * 0.25
    my = product(m, y)
    y2 = product(y, y)
    return (5.0 * y - product(product(y2, y2), my)) * 0.25, 1.0 / jnp.sqrt(jnp.sqrt(size))


def step_kernel(
    dp, mp, owners, acts_in, cots_in, update, root, graft_ref, acts, cots, in_sem, grad, oriented, a_sel, c_sel, a_all, c_all,
    stats, slots, pre, out, got,
    az_send, ax_send, am_send, cz_send, cx_send, a_recv, c_recv, d_send, d_recv, u_send, u_recv,
):
    pairs = dp // 2
    me = lax.axis_index("dp")
    col = lax.axis_index("mp")
    pair = me // 2
    side = me % 2
    across = 2 * pair + 1 - side

    def source(k):
        return 2 * lax.rem(pair + k, pairs) + side

    barrier = pltpu.get_barrier_semaphore()
    count = dp * mp
    flat = me * mp + col

    def peer(k):
        other = lax.rem(flat + k, count)
        return other // mp, lax.rem(other, mp)

    @pl.loop(1, count)
    def _(k):
        pl.semaphore_signal(barrier, inc=1, device_id=peer(k), device_id_type=MESH)


    fetches = [
        pltpu.make_async_copy(acts_in, acts, in_sem.at[0]),
        pltpu.make_async_copy(cots_in, cots, in_sem.at[1]),
    ]
    for fetch in fetches:
        fetch.start()
    for fetch in fetches:
        fetch.wait()

    def block_of(which):
        held = [jnp.where(owners[b] // 2 == which, b, 0) for b in range(owners.shape[0])]
        return functools.reduce(jnp.add, held)

    def chosen(wide, which):
        parts = [
            wide[:, n * B : (n + 1) * B] * jnp.where(which == n, 1.0, 0.0).astype(wide.dtype)
            for n in range(wide.shape[1] // B)
        ]
        return functools.reduce(jnp.add, parts)

    part = a_sel.shape[1]
    scale = 1.0 / math.sqrt(dp * cots.shape[0])
    for dest in range(pairs):
        block = block_of(dest)
        row_start = pl.multiple_of(col * part, part)
        mine = acts[pl.ds(row_start, part), :]
        a_sel[dest] = chosen(mine, block // CB)
        c_sel[dest] = chosen(cots[...], block % CB)
    is_left = functools.reduce(
        jnp.add, [jnp.where(owners[b] == me, 1.0, 0.0) for b in range(owners.shape[0])])
    a_all[me, col] = a_sel[pair]
    c_all[me] = c_sel[pair]
    pl.semaphore_wait(barrier, count - 1)

    def a_pair(k):
        dest = lax.rem(pair + k, pairs)
        return pltpu.make_async_remote_copy(
            a_sel.at[dest], a_all.at[me, col], az_send.at[k], a_recv.at[me, col], (source(k), col), MESH)

    chunk = cots.shape[0] // CHUNKS

    def c_pair(k, h):
        dest = lax.rem(pair + k, pairs)
        cut = pl.ds(h * chunk, chunk)
        return pltpu.make_async_remote_copy(
            c_sel.at[dest, cut], c_all.at[me, cut], cz_send.at[k, h], c_recv.at[me, h], (source(k), col), MESH)

    def a_across(k):
        src = source(k)
        ref = a_sel.at[pair] if k == 0 else a_all.at[src, col]
        return pltpu.make_async_remote_copy(
            ref, a_all.at[src, col], ax_send.at[k], a_recv.at[src, col], (across, col), MESH)

    def c_across(k, h):
        src = source(k)
        cut = pl.ds(h * chunk, chunk)
        ref = c_sel.at[pair, cut] if k == 0 else c_all.at[src, cut]
        return pltpu.make_async_remote_copy(
            ref, c_all.at[src, cut], cx_send.at[k, h], c_recv.at[src, h], (across, col), MESH)

    def a_mp(src, k, own=False):
        ref = a_sel.at[pair] if own else a_all.at[src, col]
        return pltpu.make_async_remote_copy(
            ref, a_all.at[src, col], am_send.at[src, k], a_recv.at[src, col], (me, lax.rem(col + k, mp)), MESH)

    def start_mp(src):
        @pl.loop(1, mp)
        def _(k):
            a_mp(src, k).start()

    def a_arrived(src, who):
        pltpu.make_async_copy(a_all.at[src, who], a_all.at[src, who], a_recv.at[src, who]).wait()

    def c_arrived(src, h):
        ref = c_all.at[src, pl.ds(h * chunk, chunk)]
        pltpu.make_async_copy(ref, ref, c_recv.at[src, h]).wait()

    order = list(range(1, pairs))
    a_across(0).start()
    for k in order:
        a_pair(k).start()
    for h in range(CHUNKS):
        c_across(0, h).start()
        for k in order:
            c_pair(k, h).start()

    @pl.loop(1, mp)
    def _(k):
        a_mp(me, k, own=True).start()

    for k in order:
        a_arrived(source(k), col)
        a_across(k).start()
        start_mp(source(k))
    for k in range(pairs):
        other = source(k) + 1 - 2 * side
        a_arrived(other, col)
        start_mp(other)
    def a_complete(src):
        @pl.loop(1, mp)
        def _(k):
            a_arrived(src, lax.rem(col + k, mp))

    def accumulate(k):
        base = 2 * lax.rem(pair + k, pairs)
        a_complete(base)
        a_complete(base + 1)
        for h in range(CHUNKS):
            c_arrived(source(k) + 1 - 2 * side, h)
        tokens = 2 * cots.shape[0]
        a = a_all[pl.ds(base, 2)].reshape(tokens, B)
        c = c_all[pl.ds(base, 2)].reshape(tokens, B)
        keep = is_left.astype(a.dtype)
        swap = (1.0 - is_left).astype(a.dtype)
        first = a * keep + c * swap
        second = c * keep + a * swap
        dims = (((0,), (0,)), ((), ()))
        add = lax.dot_general(a, c, dims, preferred_element_type=jnp.float32) * scale
        add_oriented = lax.dot_general(first, second, dims, preferred_element_type=jnp.float32) * scale
        if k == 0:
            grad[...] = add
            oriented[...] = add_oriented
        else:
            grad[...] += add
            oriented[...] += add_oriented

    for h in range(CHUNKS):
        for k in order:
            c_arrived(source(k), h)
            c_across(k, h).start()
            if h == CHUNKS - 1:
                accumulate(k - 1)
    accumulate(pairs - 1)

    g = oriented[...]
    grad_total = total(g * g)
    ids = lax.broadcasted_iota(jnp.int32, (B, B), 0), lax.broadcasted_iota(jnp.int32, (B, B), 1)
    eye = jnp.where(ids[0] == ids[1], 1.0, 0.0)
    ridge = 0.1 * (grad_total / B + 1.0)
    root[...], factor = inverse_root(product(g, g, transposed=True) + ridge * eye, eye)
    is_right = 1.0 - is_left
    halves, rows = out.shape[:2]
    starts = [pl.multiple_of((2 * h + side) * rows, rows) for h in range(halves)]
    first = jnp.concatenate(
        [root[pl.ds(n, rows), :] * is_left + grad[pl.ds(n, rows), :] * is_right for n in starts], axis=0)
    last = grad[...] * is_left + root[...] * is_right
    mine = product(product(first, root[...]), last) * (factor * factor)
    row_ids = lax.broadcasted_iota(jnp.int32, stats.shape, 0)
    stats[...] = jnp.where(row_ids == 0, 0.5 * grad_total, total(mine * mine))
    slots[me, col] = stats[...]
    pre[...] = mine.reshape(halves, rows, B)

    def share(k):
        return pltpu.make_async_remote_copy(
            stats, slots.at[me, col], d_send.at[k], d_recv.at[flat], peer(k), MESH)

    @pl.loop(1, count)
    def _(k):
        share(k).start()

    @pl.loop(1, count)
    def _(k):
        pltpu.make_async_copy(stats, stats, d_recv.at[lax.rem(flat + k, count)]).wait()

    totals = jnp.sum(slots[...].reshape(dp * mp, *stats.shape), axis=0)
    grad_total = totals[0:1, 0:1]
    pre_total = totals[1:2, 0:1]
    graft = jnp.sqrt(grad_total / jnp.maximum(pre_total, 1.0))
    graft_ref[0, 0] = graft[0, 0]
    out[...] = (pre[...] * graft[None]).astype(jnp.bfloat16)

    def piece(k):
        dest = lax.rem(pair + k, pairs)
        return pltpu.make_async_remote_copy(
            out.at[dest % halves], got.at[pair], u_send.at[k], u_recv.at[pair], (2 * dest + side, col), MESH)

    for k in range(1, pairs):
        piece(k).start()
    got[pair] = out[pair % halves]
    root[...] = root[...] * factor
    for k in range(1, pairs):
        who = lax.rem(pair + k, pairs)
        pltpu.make_async_copy(got.at[who], got.at[who], u_recv.at[who]).wait()
    for c in range(CB):
        holder = owners[(pair // halves) * CB + c] // 2
        update[:, c * B : (c + 1) * B] = got[holder]
    @pl.loop(0, dp)
    def _(src):
        @pl.loop(1, mp)
        def _(k):
            a_mp(src, k).wait_send()

    for k in range(pairs):
        a_across(k).wait_send()
        for h in range(CHUNKS):
            c_across(k, h).wait_send()
    for k in order:
        a_pair(k).wait_send()
        for h in range(CHUNKS):
            c_pair(k, h).wait_send()

    @pl.loop(1, count)
    def _(k):
        share(k).wait_send()

    for k in range(1, pairs):
        piece(k).wait_send()


def on_device(activations, cotangents, owners):
    dp = lax.axis_size("dp")
    mp = lax.axis_size("mp")
    pairs = dp // 2
    tokens, features = activations.shape
    part = tokens // mp
    rows = features // dp
    halves = B // rows // 2
    vmem = pl.BlockSpec(memory_space=pltpu.VMEM)
    smem = pl.BlockSpec(memory_space=pltpu.SMEM)
    hbm = pl.BlockSpec(memory_space=pltpu.HBM)
    dma = pltpu.SemaphoreType.DMA
    update, root, graft = pl.pallas_call(
        functools.partial(step_kernel, dp, mp),
        out_shape=(
            jax.ShapeDtypeStruct((rows, CB * B), jnp.bfloat16),
            jax.ShapeDtypeStruct((B, B), jnp.float32),
            jax.ShapeDtypeStruct((1, 1), jnp.float32),
        ),
        in_specs=[smem, hbm, hbm],
        out_specs=(vmem, vmem, smem),
        scratch_shapes=[
            pltpu.VMEM(activations.shape, jnp.bfloat16),
            pltpu.VMEM(cotangents.shape, jnp.bfloat16),
            dma((2,)),
            pltpu.VMEM((B, B), jnp.float32),
            pltpu.VMEM((B, B), jnp.float32),
            pltpu.VMEM((pairs, part, B), jnp.bfloat16),
            pltpu.VMEM((pairs, tokens, B), jnp.bfloat16),
            pltpu.VMEM((dp, mp, part, B), jnp.bfloat16),
            pltpu.VMEM((dp, tokens, B), jnp.bfloat16),
            pltpu.VMEM((8, 128), jnp.float32),
            pltpu.VMEM((dp, mp, 8, 128), jnp.float32),
            pltpu.VMEM((halves, rows, B), jnp.float32),
            pltpu.VMEM((halves, rows, B), jnp.bfloat16),
            pltpu.VMEM((pairs, rows, B), jnp.bfloat16),
            dma((pairs,)), dma((pairs,)), dma((dp, mp)), dma((pairs, CHUNKS)), dma((pairs, CHUNKS)), dma((dp, mp)), dma((dp, CHUNKS)),
            dma((dp * mp,)), dma((dp * mp,)), dma((pairs,)), dma((pairs,)),
        ],
        compiler_params=pltpu.CompilerParams(collective_id=0, has_side_effects=True, vmem_limit_bytes=48 * 1024 * 1024),
    )(owners, activations, cotangents)
    return (update, root, graft[0, 0])


def solution(mesh):
    return jax.shard_map(
        on_device,
        mesh=mesh,
        in_specs=(P("dp", None), P("dp", "mp"), P()),
        out_specs=(P("dp", "mp"), P("dp", "mp"), P()),
        check_vma=False,
    )
```
